32 devices in a mesh: trunk: 4 (over x, core), branch: 8 (over z, y).
Axes of the slice: x: 2, y: 2, z: 4, core: 2. Of those that a mesh axis runs over, the one named last changes fastest.
Arguments:
- queries: bfloat16 [4, 1024, 4096], P('trunk', 'branch'), may hold values from -160 to 160
- keys_values: bfloat16 [4, 1024, 2, 512], P('trunk', 'branch'), may hold values from -7 to 7
- out_grad: bfloat16 [4, 1024, 4096], P('trunk', 'branch'), may hold values from -6 to 6
- trunk_kv: bfloat16 [4, 8, 2, 16, 512], P('trunk', 'branch'), may hold values from -6 to 6
- branch_of: int32 [4, 1024], P('trunk', 'branch'), may hold values from 0 to 15, never falling along the last dimension, each value on 1 to 128 neighbouring positions
- branch_reach: int32 [4, 16], P('trunk'), may hold values from 1 to 4
- ancestors: int32 [4, 8, 4], P('trunk', 'branch'), may hold values from 0 to 7
Outputs:
- attended: bfloat16 [4, 1024, 4096], P('trunk', 'branch')
- query_grad: bfloat16 [4, 1024, 4096], P('trunk', 'branch')
- kv_grad: float32 [4, 1024, 2, 512], P('trunk', 'branch')
- trunk_grad: float32 [4, 8, 2, 16, 512], P('trunk', 'branch')
The draws below stay inside these ranges and needn't reach their ends.
Inputs may be any that keep to these rules, and one draw needn't show every extreme that they name: `branch_of`: ids never fall along a row; each branch covers 1 to 128 consecutive tokens. `ancestors`: entry d names the branch index of the device at trunk index d that holds the segment read at depth d.
All inputs are finite; a program needn't handle non-finite values.
Results may differ from the reference program's by a relative error of at most 0.005.
Values may be sent and summed in bfloat16 or wider, within the bound.
No kernel may reach another device: no remote copies, remote signals or barrier semaphores. Data moves between devices by JAX's collectives and lax.ppermute only.
A program may use at most 128 MiB of HBM per device.

```python
import math
import jax
import jax.numpy as jnp
import numpy as np
from jax import lax

HQ = 32
KVH = 4
DH = 128
Q_DEV = 128
SEG_LEN = 16
DEPTHS = 4
S_ROW = 1024
BRANCHES = 16
N_TRUNK = 4
N_BRANCH = 8


def shared_fields(key):
    base = jax.random.fold_in(key, 91)
    first_key, second_key, third_key = jax.random.split(base, 3)
    width = KVH * DH
    key_field = jnp.clip(jax.random.normal(first_key, (N_TRUNK, S_ROW, width), jnp.float32), -6.0, 6.0)
    value_field = jnp.clip(jax.random.normal(second_key, (N_TRUNK, S_ROW, width), jnp.float32), -6.0, 6.0)
    query_field = jnp.clip(jax.random.normal(third_key, (N_TRUNK, S_ROW, HQ * DH), jnp.float32), -6.0, 6.0)
    return (query_field, jnp.stack([key_field, value_field], axis=2))


def draw_queries(key, part):
    return shared_fields(key)[0].astype(jnp.bfloat16)


def draw_keys_values(key, part):
    return shared_fields(key)[1].astype(jnp.bfloat16)


def touch_ends(drawn, stream_key, smallest, high):
    longest = drawn.shape.index(max(drawn.shape))
    spots = []
    for shift in (0, 1):
        where = [jax.random.randint(jax.random.fold_in(stream_key, axis), (), 0, length) for axis, length in enumerate(drawn.shape)]
        where[longest] = (where[longest] + shift) % drawn.shape[longest]
        spots.append(tuple(where))
    return drawn.at[spots[0]].set(smallest).at[spots[1]].set(high)


def block_scale(stream_key, dims, cuts, low, top_value):
    gain = 1.0
    for axis_at, shards_of in cuts:
        steps = jax.random.uniform(jax.random.fold_in(jax.random.fold_in(stream_key, 6), axis_at), (shards_of,), jnp.float32, low / len(cuts), top_value / len(cuts))
        gain = gain * jnp.repeat(jnp.exp(steps), dims[axis_at] // shards_of).reshape((-1,) + (1,) * (len(dims) - 1 - axis_at))
    return gain


def rank_table(number_of, slope):
    portions = [(1 << 20) // math.isqrt(grade ** slope) + 1 for grade in range(1, number_of + 1)]
    scale = 1 + sum(portions) // (1 << 30)
    return np.cumsum(np.array([max(1, weight // scale) for weight in portions]))


def skewed_ids(key, extent, number_of, lean):
    table = rank_table(number_of, lean)
    lot = jax.random.randint(jax.random.fold_in(key, 1), extent, 0, int(table[number_of - 1]))
    grade = jnp.searchsorted(jnp.asarray(table, jnp.int32), lot, side="right")
    return jax.random.permutation(jax.random.fold_in(key, 2), number_of)[grade].astype(jnp.int32)


def length_profile(count, total, most, skew):
    weights = [(1 << 20) // math.isqrt(rank ** skew) + 1 for rank in range(2, count + 1)]
    surplus, counts = total - most - (count - 1), [1] * (count - 1)
    while surplus > 0:
        free = [i for i in range(count - 1) if counts[i] < most]
        pool, left = sum([weights[i] for i in free]), surplus
        for i in free:
            addition = min(most - counts[i], max(1, left * weights[i] // pool), surplus)
            counts[i] = counts[i] + addition
            surplus = surplus - addition
    return np.array([most] + counts)


def uneven_parts(stream_key, number_of, total, limit, slope):
    if number_of == 2:
        one = jax.random.randint(stream_key, (), max(1, total - limit), min(limit, total - 1) + 1)
        return jnp.stack([one, total - one])
    sizes = jnp.asarray(length_profile(number_of, total, limit, slope), jnp.int32)
    pairs = (number_of - 1) // 2
    donor, receiver = sizes[1:1 + 2 * pairs:2], sizes[2:2 + 2 * pairs:2]
    margin = jnp.minimum(donor - 1, limit - receiver)
    moved = jax.random.randint(jax.random.fold_in(stream_key, 1), (pairs,), 0, 1 << 20) % (margin + 1)
    sizes = sizes.at[1:1 + 2 * pairs:2].set(donor - moved).at[2:2 + 2 * pairs:2].set(receiver + moved)
    return sizes[jax.random.permutation(jax.random.fold_in(stream_key, 2), number_of)]


def centred(stream_key, extent, scale, limit, cuts=(), held_as=jnp.bfloat16):
    drawn = scale * jax.random.normal(stream_key, extent, jnp.float32)
    if cuts:
        drawn = drawn * block_scale(stream_key, extent, cuts, -0.22, 0.18)
    return jnp.clip(drawn, -limit, limit).astype(held_as)


def setup_inputs(seed: int = 0) -> dict:
    seeds = jax.random.split(jax.random.key(seed), 8)
    return {
        "queries": draw_queries(jax.random.fold_in(seeds[7], 71), 0),
        "keys_values": draw_keys_values(jax.random.fold_in(seeds[7], 71), 0),
        "out_grad": centred(seeds[2], (N_TRUNK, S_ROW, HQ * DH), 1.0, 6.0, ((0, 4), (1, 8))),
        "trunk_kv": centred(seeds[3], (DEPTHS, N_BRANCH, 2, SEG_LEN, KVH * DH), 1.0, 6.0, ((0, 4), (1, 8))),
        "branch_of": jax.vmap(lambda own: jnp.searchsorted(jnp.cumsum(uneven_parts(own, BRANCHES, S_ROW, Q_DEV, 2)), jnp.arange(S_ROW), side="right"))(jax.random.split(seeds[4], N_TRUNK)).reshape((N_TRUNK, S_ROW)).astype(jnp.int32),
        "branch_reach": touch_ends(jax.random.randint(seeds[5], (N_TRUNK, BRANCHES), 1, DEPTHS + 1), jax.random.fold_in(seeds[5], 1), 1, DEPTHS).astype(jnp.int32),
        "ancestors": touch_ends(skewed_ids(seeds[6], (N_TRUNK, N_BRANCH, DEPTHS), N_BRANCH, 2), jax.random.fold_in(seeds[6], 3), 0, N_BRANCH - 1).astype(jnp.int32),
    }


def build_allowed(tags, earlier_tags, reach_rows, seg_len, depth_count):
    trunk_depth = jnp.arange(depth_count * seg_len, dtype=jnp.int32) // seg_len
    trunk_ok = trunk_depth[None, :] < reach_rows[:, None]
    earlier_ok = earlier_tags[None, :] == tags[:, None]
    position = jnp.arange(tags.shape[0], dtype=jnp.int32)
    own_ok = (tags[None, :] == tags[:, None]) & (position[None, :] <= position[:, None])
    return jnp.concatenate([trunk_ok, earlier_ok, own_ok], axis=1)

def attend_block(query_rows, grad_rows, key_rows, value_rows, allowed):
    head_scale = 1.0 / math.sqrt(DH)
    group = HQ // KVH
    n_rows = query_rows.shape[0]
    outputs, query_grads, key_grads, value_grads = ([], [], [], [])
    for head_group in range(KVH):
        query_part = query_rows[:, head_group * group * DH:(head_group + 1) * group * DH].reshape(n_rows, group, DH).astype(jnp.float32)
        grad_part = grad_rows[:, head_group * group * DH:(head_group + 1) * group * DH].reshape(n_rows, group, DH).astype(jnp.float32)
        key_part = key_rows[:, head_group * DH:(head_group + 1) * DH].astype(jnp.float32)
        value_part = value_rows[:, head_group * DH:(head_group + 1) * DH].astype(jnp.float32)
        scores = jnp.einsum('qrd,kd->rqk', query_part, key_part) * head_scale
        masked = jnp.where(allowed[None], scores, -1e+30)
        highest = lax.optimization_barrier(jnp.max(masked, axis=-1, keepdims=True))
        expo = jnp.exp(masked - highest)
        weights = expo / lax.optimization_barrier(jnp.sum(expo, axis=-1, keepdims=True))
        weights_bf = weights.astype(jnp.bfloat16).astype(jnp.float32)
        output = jnp.einsum('rqk,kd->qrd', weights_bf, value_part).reshape(n_rows, group * DH)
        grad_weights = jnp.einsum('qrd,kd->rqk', grad_part, value_part)
        row_mean = lax.optimization_barrier(jnp.sum(weights * grad_weights, axis=-1, keepdims=True))
        score_grad = (weights * (grad_weights - row_mean)).astype(jnp.bfloat16).astype(jnp.float32)
        outputs.append(output)
        query_grads.append((jnp.einsum('rqk,kd->qrd', score_grad, key_part) * head_scale).reshape(n_rows, group * DH))
        key_grads.append(jnp.einsum('rqk,qrd->kd', score_grad, query_part) * head_scale)
        value_grads.append(jnp.einsum('rqk,qrd->kd', weights_bf, grad_part))
    attended = jnp.concatenate(outputs, axis=1).astype(jnp.bfloat16)
    query_grad = jnp.concatenate(query_grads, axis=1).astype(jnp.bfloat16)
    return (attended, query_grad, jnp.concatenate(key_grads, axis=1), jnp.concatenate(value_grads, axis=1))

def reference(queries, keys_values, out_grad, trunk_kv, branch_of, branch_reach, ancestors):
    width = KVH * DH
    depth_index = jnp.arange(DEPTHS, dtype=jnp.int32)
    trunk_len = DEPTHS * SEG_LEN
    zero_index = jnp.zeros((), jnp.int32)

    def one_block(carry, block_index):
        trunk_acc, branch_acc = carry
        row = (block_index // N_BRANCH).astype(jnp.int32)
        column = (block_index % N_BRANCH).astype(jnp.int32)
        first_row = (column * Q_DEV).astype(jnp.int32)
        has_earlier = column > 0
        earlier_first = jnp.maximum(first_row - Q_DEV, 0).astype(jnp.int32)
        query_rows = lax.dynamic_slice(queries, (row, first_row, zero_index), (1, Q_DEV, HQ * DH))[0]
        grad_rows = lax.dynamic_slice(out_grad, (row, first_row, zero_index), (1, Q_DEV, HQ * DH))[0]
        own_kv = lax.dynamic_slice(keys_values, (row, first_row, zero_index, zero_index), (1, Q_DEV, 2, width))[0]
        earlier_kv = lax.dynamic_slice(keys_values, (row, earlier_first, zero_index, zero_index), (1, Q_DEV, 2, width))[0]
        earlier_kv = jnp.where(has_earlier, earlier_kv, jnp.zeros_like(earlier_kv))
        branch_ids = lax.dynamic_slice(branch_of, (row, first_row), (1, Q_DEV))[0]
        earlier_ids = lax.dynamic_slice(branch_of, (row, earlier_first), (1, Q_DEV))[0]
        tags = branch_ids + 1
        earlier_tags = jnp.where(has_earlier, earlier_ids + 1, jnp.zeros_like(earlier_ids))
        reach_table = lax.dynamic_slice(branch_reach, (row, zero_index), (1, BRANCHES))[0]
        branch_index = jnp.arange(BRANCHES, dtype=jnp.int32)
        reach_rows = lax.optimization_barrier(jnp.sum(jnp.where(branch_ids[:, None] == branch_index[None, :], reach_table[None, :], 0), axis=1)).astype(jnp.int32)
        owners = lax.dynamic_slice(ancestors, (row, column, zero_index), (1, 1, DEPTHS))[0, 0]
        fetched = trunk_kv[depth_index, owners]
        key_rows = jnp.concatenate([fetched[:, 0].reshape(trunk_len, width), earlier_kv[:, 0], own_kv[:, 0]], axis=0)
        value_rows = jnp.concatenate([fetched[:, 1].reshape(trunk_len, width), earlier_kv[:, 1], own_kv[:, 1]], axis=0)
        allowed = build_allowed(tags, earlier_tags, reach_rows, SEG_LEN, DEPTHS)
        attended, query_grad, key_grad, value_grad = attend_block(query_rows, grad_rows, key_rows, value_rows, allowed)
        trunk_part = jnp.stack([key_grad[:trunk_len].reshape(DEPTHS, SEG_LEN, width), value_grad[:trunk_len].reshape(DEPTHS, SEG_LEN, width)], axis=1)
        trunk_acc = trunk_acc.at[depth_index, owners].add(trunk_part)
        earlier_part = jnp.stack([key_grad[trunk_len:trunk_len + Q_DEV], value_grad[trunk_len:trunk_len + Q_DEV]], axis=1)
        earlier_part = jnp.where(has_earlier, earlier_part, jnp.zeros_like(earlier_part))
        own_part = jnp.stack([key_grad[trunk_len + Q_DEV:], value_grad[trunk_len + Q_DEV:]], axis=1)
        current = lax.dynamic_slice(branch_acc, (row, earlier_first, zero_index, zero_index), (1, Q_DEV, 2, width))
        branch_acc = lax.dynamic_update_slice(branch_acc, current + earlier_part[None], (row, earlier_first, zero_index, zero_index))
        current = lax.dynamic_slice(branch_acc, (row, first_row, zero_index, zero_index), (1, Q_DEV, 2, width))
        branch_acc = lax.dynamic_update_slice(branch_acc, current + own_part[None], (row, first_row, zero_index, zero_index))
        return ((trunk_acc, branch_acc), (attended, query_grad))
    start_carry = (jnp.zeros(trunk_kv.shape, jnp.float32), jnp.zeros(keys_values.shape, jnp.float32))
    (trunk_acc, branch_acc), (attended, query_grad) = lax.scan(one_block, start_carry, jnp.arange(N_TRUNK * N_BRANCH, dtype=jnp.int32))
    attended = attended.reshape(N_TRUNK, S_ROW, HQ * DH)
    query_grad = query_grad.reshape(N_TRUNK, S_ROW, HQ * DH)
    return (attended, query_grad, branch_acc, trunk_acc)
```

```python
import functools
import math

import jax
import jax.numpy as jnp
from jax import lax
from jax.experimental import pallas as pl
from jax.experimental.pallas import tpu as pltpu
from jax.sharding import PartitionSpec as P

HQ = 32
KVH = 4
DH = 128
GROUP = HQ // KVH
BF = jnp.bfloat16
F32 = jnp.float32


def shift(block, axis, distance):
    devices = range(lax.axis_size(axis))
    route = [(i - distance, i) for i in devices if i - distance in devices]
    return lax.ppermute(block, axis, route)


def dot(a, b, ca, cb):
    return lax.dot_general(a, b, (((ca,), (cb,)), ((), ())), preferred_element_type=F32)


def build_allowed(reach_ref, tags_ref, n, trunk_len, seg_len):
    tag_row = tags_ref[0:1, :]
    earlier_row = tags_ref[1:2, :]
    reach_row = jnp.zeros((1, n), jnp.int32)
    for b in range(reach_ref.shape[0]):
        reach_row = jnp.where(tag_row == b + 1, reach_ref[b], reach_row)
    tag_cols = jnp.broadcast_to(tag_row, (n, n))
    key_tags = tag_cols.T
    earlier_tags = jnp.broadcast_to(earlier_row, (n, n)).T
    k_idx = lax.broadcasted_iota(jnp.int32, (n, n), 0)
    q_idx = lax.broadcasted_iota(jnp.int32, (n, n), 1)
    depth = lax.broadcasted_iota(jnp.int32, (trunk_len, n), 0) // seg_len
    trunk_ok = depth < jnp.broadcast_to(reach_row, (trunk_len, n))
    earlier_ok = earlier_tags == tag_cols
    own_ok = (key_tags == tag_cols) & (k_idx <= q_idx)
    as_float = [jnp.where(ok, 0.0, -1e30).astype(F32) for ok in (trunk_ok, earlier_ok, own_ok)]
    return jnp.concatenate(as_float, axis=0)


def attend_kernel(
    reach_ref, tags_ref, q_ref, g_ref, trunk_ref, ek_ref, ev_ref, ok_ref, ov_ref,
    out_ref, dq_ref, dtrunk_ref, dearlier_ref, down_ref, bias_ref,
):
    n = q_ref.shape[0]
    depths, _, seg_len, _ = trunk_ref.shape
    trunk_len = depths * seg_len
    scale = 1.0 / math.sqrt(DH)

    @pl.when(pl.program_id(0) == 0)
    def _():
        bias_ref[...] = build_allowed(reach_ref, tags_ref, n, trunk_len, seg_len)

    keys = jnp.concatenate(
        [trunk_ref[:, 0].reshape(trunk_len, DH), ek_ref[...], ok_ref[...]], axis=0
    )
    values = jnp.concatenate(
        [trunk_ref[:, 1].reshape(trunk_len, DH), ev_ref[...], ov_ref[...]], axis=0
    )
    q_rows = jnp.concatenate([q_ref[:, r * DH : (r + 1) * DH] for r in range(GROUP)], axis=0)
    g_rows = jnp.concatenate([g_ref[:, r * DH : (r + 1) * DH] for r in range(GROUP)], axis=0)
    bias = jnp.concatenate([bias_ref[...]] * GROUP, axis=1)
    scores = dot(keys, q_rows, 1, 1) * scale + bias
    grad_w = dot(values, g_rows, 1, 1)
    highest = jnp.max(scores, axis=0, keepdims=True)
    expo = jnp.exp(scores - highest)
    weights = expo * (1.0 / jnp.sum(expo, axis=0, keepdims=True))
    weights_bf = weights.astype(BF)
    row_mean = jnp.sum(weights * grad_w, axis=0, keepdims=True)
    score_grad = (weights * (grad_w - row_mean)).astype(BF)
    out_t = dot(values, weights_bf, 0, 0)
    dq_t = dot(keys, score_grad, 0, 0) * scale
    for r in range(GROUP):
        cols = slice(r * n, (r + 1) * n)
        out_ref[:, r * DH : (r + 1) * DH] = out_t[:, cols].T.astype(BF)
        dq_ref[:, r * DH : (r + 1) * DH] = dq_t[:, cols].T.astype(BF)
    for which, grad in enumerate(
        (dot(score_grad, q_rows, 1, 0) * scale, dot(weights_bf, g_rows, 1, 0))
    ):
        dtrunk_ref[:, which] = grad[:trunk_len].reshape(depths, seg_len, DH).astype(BF)
        dearlier_ref[which] = grad[trunk_len : trunk_len + n].astype(BF)
        down_ref[which] = grad[trunk_len + n :]


def attend(reach, tags, q, g, trunk, earlier, own):
    n, width = q.shape
    depths, _, seg_len, kv_width = trunk.shape
    heads = kv_width // DH
    part = width // heads
    wide = pl.BlockSpec((n, part), lambda h: (0, h))
    kspec = pl.BlockSpec((n, DH), lambda h: (0, h))
    vspec = pl.BlockSpec((n, DH), lambda h: (0, h + heads))
    tspec = pl.BlockSpec((depths, 2, seg_len, DH), lambda h: (0, 0, 0, h))
    kvspec = pl.BlockSpec((2, n, DH), lambda h: (0, 0, h))
    return pl.pallas_call(
        attend_kernel,
        grid=(heads,),
        in_specs=[
            pl.BlockSpec(memory_space=pltpu.SMEM),
            pl.BlockSpec((2, n), lambda h: (0, 0)),
            wide, wide, tspec, kspec, vspec, kspec, vspec,
        ],
        out_specs=[wide, wide, tspec, kvspec, kvspec],
        out_shape=[
            jax.ShapeDtypeStruct((n, width), BF),
            jax.ShapeDtypeStruct((n, width), BF),
            jax.ShapeDtypeStruct(trunk.shape, BF),
            jax.ShapeDtypeStruct((2, n, kv_width), BF),
            jax.ShapeDtypeStruct((2, n, kv_width), F32),
        ],
        scratch_shapes=[pltpu.VMEM((depths * seg_len + 2 * n, n), F32)],
        name="attend",
    )(reach, tags, q, g, trunk, earlier, earlier, own, own)


def on_device(queries, keys_values, out_grad, trunk_kv, branch_of, branch_reach, ancestors):
    depth_count = lax.axis_size("trunk")
    n_branch = lax.axis_size("branch")
    block_len = queries.shape[1]
    requested = lax.all_to_all(ancestors[0, 0], "trunk", split_axis=0, concat_axis=0, tiled=True)
    own_segment = trunk_kv[0]
    copies = jnp.broadcast_to(own_segment, (n_branch,) + own_segment.shape[1:])
    piece = lax.all_to_all(copies, "branch", split_axis=0, concat_axis=0, tiled=True)
    owner_index = jnp.arange(n_branch, dtype=jnp.int32)
    hits = (requested[:, None] == owner_index[None, :]).astype(BF)
    picked = jnp.einsum("tn,nslc->tslc", hits, piece, preferred_element_type=F32).astype(BF)
    fetched = lax.all_to_all(picked, "trunk", split_axis=0, concat_axis=0, tiled=True)
    tags = branch_of[0] + 1
    own_kv = keys_values[0].reshape(block_len, -1)
    earlier_kv, earlier_tags = shift((own_kv, tags), "branch", 1)
    attended, query_grad, trunk_part, earlier_part, own_part = attend(
        branch_reach[0], jnp.stack([tags, earlier_tags]), queries[0], out_grad[0],
        fetched, earlier_kv, own_kv,
    )
    from_next = shift(earlier_part, "branch", -1)
    returned = lax.all_to_all(trunk_part, "trunk", split_axis=0, concat_axis=0, tiled=True)
    owners_hit = (requested[None, :] == owner_index[:, None]).astype(BF)
    dense = jnp.einsum("ot,tslc->oslc", owners_hit, returned, preferred_element_type=F32).astype(BF)
    parts = lax.all_to_all(dense, "branch", split_axis=0, concat_axis=0, tiled=True)
    trunk_grad = jnp.sum(parts.astype(F32), axis=0)[None, None]
    kv_grad = jnp.swapaxes(own_part + from_next.astype(F32), 0, 1)[None]
    return (attended[None], query_grad[None], kv_grad, trunk_grad)


def solution(mesh):
    return jax.shard_map(
        on_device,
        mesh=mesh,
        in_specs=(
            P("trunk", "branch", None),
            P("trunk", "branch", None, None),
            P("trunk", "branch", None),
            P("trunk", "branch", None, None, None),
            P("trunk", "branch"),
            P("trunk", None),
            P("trunk", "branch", None),
        ),
        out_specs=(
            P("trunk", "branch", None),
            P("trunk", "branch", None),
            P("trunk", "branch", None, None),
            P("trunk", "branch", None, None, None),
        ),
        check_vma=False,
    )
```

```python
import functools
import math

import jax
import jax.numpy as jnp
from jax import lax
from jax.experimental import pallas as pl
from jax.experimental.pallas import tpu as pltpu
from jax.sharding import PartitionSpec as P


HQ = 32
KVH = 4
DH = 128
GROUP = HQ // KVH
SCALE = 1.0 / math.sqrt(DH)
LOG2E = 1.0 / math.log(2.0)
BF = jnp.bfloat16
F32 = jnp.float32
PACK = 16
GATHER_FIRST = []
SCATTER_FIRST = [1]
VMEM_LIMIT = 24 * 1024 * 1024


def ring(block, axis, distance):
    size = lax.axis_size(axis)
    return lax.ppermute(block, axis, [(i, (i + distance) % size) for i in range(size)])


def swap(block, axis, k):
    if k == 0:
        return block
    return lax.ppermute(block, axis, [(i, i ^ k) for i in range(lax.axis_size(axis))])


def dot(a, b, ca, cb):
    return lax.dot_general(a, b, (((ca,), (cb,)), ((), ())), preferred_element_type=F32)


def head_rows(ref, h):
    first = h * GROUP
    return jnp.concatenate(
        [ref[:, (first + r) * DH : (first + r + 1) * DH] for r in range(GROUP)], axis=0
    )


def tile_heads(x):
    return jnp.concatenate([x] * GROUP, axis=1)


def as_bias(ok):
    return jnp.where(ok, 0.0, -1e30).astype(F32)


def cols(h):
    return slice(h * DH, (h + 1) * DH)


def call(kernel, outs, *args, hbm=0, hbm_outs=0, scratch=(), aliases={}):
    vspec = pl.BlockSpec(memory_space=pltpu.VMEM)
    hspec = pl.BlockSpec(memory_space=pltpu.HBM)
    places = [pltpu.HBM] * hbm + [pltpu.VMEM] * (len(args) - hbm)
    args = [pltpu.with_memory_space_constraint(a, p) for a, p in zip(args, places)]
    shapes = [jax.ShapeDtypeStruct(shape, dtype) for shape, dtype in outs[:hbm_outs]]
    shapes += [pltpu.VMEM(shape, dtype) for shape, dtype in outs[hbm_outs:]]
    return pl.pallas_call(
        kernel,
        in_specs=[hspec] * hbm + [vspec] * (len(args) - hbm),
        out_specs=[hspec] * hbm_outs + [vspec] * (len(outs) - hbm_outs),
        out_shape=shapes,
        scratch_shapes=scratch,
        input_output_aliases=aliases,
        compiler_params=pltpu.CompilerParams(vmem_limit_bytes=VMEM_LIMIT),
        cost_estimate=pl.CostEstimate(flops=10**8, transcendentals=0, bytes_accessed=10**5),
    )(*args)


def join_kernel(a_ref, b_ref, out_ref):
    count = a_ref.shape[0]
    out_ref[:count] = a_ref[...]
    out_ref[count:] = b_ref[...]


def prepare_kernel(
    ids_hbm, reach_hbm, owners_hbm, q_hbm, g_hbm, seg_hbm, kv_ref,
    ids_ref, owners_ref, q_ref, g_ref, seg_ref, payload_ref, tbias_ref, reach_ref, sems,
):
    copies = [
        pltpu.make_async_copy(src, dst, sems.at[i])
        for i, (src, dst) in enumerate(
            (
                (ids_hbm, ids_ref), (reach_hbm, reach_ref), (owners_hbm, owners_ref),
                (seg_hbm, seg_ref), (q_hbm, q_ref), (g_hbm, g_ref),
            )
        )
    ]
    for copy in copies:
        copy.start()
    n = kv_ref.shape[0]
    payload_ref[:n] = kv_ref[...]
    payload_ref[n:] = jnp.zeros((PACK, kv_ref.shape[1]), BF)
    copies[0].wait()
    copies[1].wait()
    ids = ids_ref[...]
    payload_ref[n:, 0:n] = jnp.broadcast_to((ids + 1).astype(F32), (PACK, n)).astype(BF)
    reach_row = jnp.zeros((1, n), jnp.int32)
    for b in range(reach_ref.shape[1]):
        reach_row = jnp.where(ids == b, reach_ref[0:1, b : b + 1], reach_row)
    depths = lax.axis_size("trunk")
    seg_len = tbias_ref.shape[0] // depths
    me = lax.axis_index("trunk")
    for k in range(depths):
        row = as_bias((me ^ k) < reach_row)
        tbias_ref[k * seg_len : (k + 1) * seg_len] = jnp.broadcast_to(row, (seg_len, n))
    for copy in copies[2:]:
        copy.wait()


def scored(keys, values, q_rows, g_rows, bias):
    return dot(keys, q_rows, 1, 1) * (SCALE * LOG2E) + bias, dot(values, g_rows, 1, 1)


def own_kernel(ids_ref, q_ref, g_ref, kv_ref, stats_ref, bias_ref):
    n = q_ref.shape[0]
    heads = stats_ref.shape[0]
    id_cols = jnp.broadcast_to(ids_ref[...].astype(F32), (n, n))
    k_idx = lax.broadcasted_iota(jnp.int32, (n, n), 0)
    q_idx = lax.broadcasted_iota(jnp.int32, (n, n), 1)
    bias_ref[...] = as_bias((id_cols.T == id_cols) & (k_idx <= q_idx))
    bias = tile_heads(bias_ref[...])
    for h in range(heads):
        scores, grad_w = scored(
            kv_ref[:n, cols(h)], kv_ref[:n, cols(h + heads)],
            head_rows(q_ref, h), head_rows(g_ref, h), bias,
        )
        highest = jnp.max(scores, axis=0, keepdims=True)
        expo = jnp.exp2(scores - highest)
        stats_ref[h, 0:1] = highest
        stats_ref[h, 1:2] = jnp.sum(expo, axis=0, keepdims=True)
        stats_ref[h, 2:3] = jnp.sum(expo * grad_w, axis=0, keepdims=True)


def merge(stats_ref, h, scores, grad_w):
    first = stats_ref[h, 0:1]
    highest = jnp.maximum(jnp.max(scores, axis=0, keepdims=True), first)
    expo = jnp.exp2(scores - highest)
    factor = jnp.exp2(first - highest)
    total = jnp.sum(expo, axis=0, keepdims=True) + stats_ref[h, 1:2] * factor
    weighted = jnp.sum(expo * grad_w, axis=0, keepdims=True) + stats_ref[h, 2:3] * factor
    return highest, expo, total, weighted


def earlier_kernel(ids_ref, q_ref, g_ref, kv_ref, stats_ref, merged_ref, bias_ref):
    n = q_ref.shape[0]
    heads = stats_ref.shape[0]
    tag_cols = jnp.broadcast_to(ids_ref[...].astype(F32) + 1.0, (n, n))
    present = (lax.axis_index("branch") > 0).astype(F32)
    earlier_row = kv_ref[n : n + 1, 0:n].astype(F32) * present
    bias_ref[...] = as_bias(jnp.broadcast_to(earlier_row, (n, n)).T == tag_cols)
    bias = tile_heads(bias_ref[...])
    for h in range(heads):
        scores, grad_w = scored(
            kv_ref[:n, cols(h)], kv_ref[:n, cols(h + heads)],
            head_rows(q_ref, h), head_rows(g_ref, h), bias,
        )
        highest, _, total, weighted = merge(stats_ref, h, scores, grad_w)
        merged_ref[h, 0:1] = highest
        merged_ref[h, 1:2] = total
        merged_ref[h, 2:3] = weighted


def trunk_kernel(q_ref, g_ref, stats_ref, tbias_ref, *refs):
    count = len(refs) // 2
    seg_refs, final_ref, dseg_refs = refs[:count], refs[count], refs[count + 1 :]
    seg_len = seg_refs[0].shape[1]
    bias = tile_heads(tbias_ref[...])
    for h in range(stats_ref.shape[0]):
        keys = jnp.concatenate([s[0, :, cols(h)] for s in seg_refs], axis=0)
        values = jnp.concatenate([s[1, :, cols(h)] for s in seg_refs], axis=0)
        q_rows = head_rows(q_ref, h)
        g_rows = head_rows(g_ref, h)
        scores, grad_w = scored(keys, values, q_rows, g_rows, bias)
        highest, expo, total, weighted = merge(stats_ref, h, scores, grad_w)
        inverse = 1.0 / total
        row_mean = weighted * inverse
        weights = expo * inverse
        score_grad = (weights * (grad_w - row_mean)).astype(BF)
        dkey = (dot(score_grad, q_rows, 1, 0) * SCALE).astype(BF)
        dvalue = dot(weights.astype(BF), g_rows, 1, 0).astype(BF)
        for k, ref in enumerate(dseg_refs):
            ref[0, :, cols(h)] = dkey[k * seg_len : (k + 1) * seg_len]
            ref[1, :, cols(h)] = dvalue[k * seg_len : (k + 1) * seg_len]
        final_ref[h, 0:1] = highest
        final_ref[h, 1:2] = inverse
        final_ref[h, 2:3] = row_mean


def finish(final_ref, h, scores, grad_w):
    weights = jnp.exp2(scores - final_ref[h, 0:1]) * final_ref[h, 1:2]
    return weights.astype(BF), (weights * (grad_w - final_ref[h, 2:3])).astype(BF)


def earlier_grad_kernel(q_ref, g_ref, final_ref, kv_ref, bias_ref, dkv_ref):
    n = q_ref.shape[0]
    heads = final_ref.shape[0]
    bias = tile_heads(bias_ref[...])
    for h in range(heads):
        q_rows = head_rows(q_ref, h)
        g_rows = head_rows(g_ref, h)
        scores, grad_w = scored(
            kv_ref[:n, cols(h)], kv_ref[:n, cols(h + heads)], q_rows, g_rows, bias
        )
        weights_bf, score_grad = finish(final_ref, h, scores, grad_w)
        dkv_ref[0, :, cols(h)] = (dot(score_grad, q_rows, 1, 0) * SCALE).astype(BF)
        dkv_ref[1, :, cols(h)] = dot(weights_bf, g_rows, 1, 0).astype(BF)


def rest_kernel(
    *refs, some, aliased
):
    refs = refs[2:] if aliased else refs
    q_ref, g_ref, final_ref, ekv_ref, kv_ref, obias_ref, ebias_ref, tbias_ref = refs[:8]
    seg_refs = refs[8:-6]
    out_hbm, dq_hbm, dkv_ref, out_ref, dq_ref, sems = refs[-6:]
    n = q_ref.shape[0]
    heads = final_ref.shape[0]
    part = GROUP * DH
    bias = tile_heads(jnp.concatenate([obias_ref[...], ebias_ref[...], tbias_ref[...]], axis=0))
    copies = []
    for i, h in enumerate(some):
        keys = jnp.concatenate(
            [kv_ref[:n, cols(h)], ekv_ref[:n, cols(h)]] + [s[0, :, cols(h)] for s in seg_refs],
            axis=0,
        )
        values = jnp.concatenate(
            [kv_ref[:n, cols(h + heads)], ekv_ref[:n, cols(h + heads)]]
            + [s[1, :, cols(h)] for s in seg_refs],
            axis=0,
        )
        q_rows = head_rows(q_ref, h)
        g_rows = head_rows(g_ref, h)
        scores, grad_w = scored(keys, values, q_rows, g_rows, bias)
        weights_bf, score_grad = finish(final_ref, h, scores, grad_w)
        out_t = dot(values, weights_bf, 0, 0)
        dq_t = dot(keys, score_grad, 0, 0) * SCALE
        for r in range(GROUP):
            rows = slice(r * n, (r + 1) * n)
            out_ref[i, :, cols(r)] = out_t[:, rows].T.astype(BF)
            dq_ref[i, :, cols(r)] = dq_t[:, rows].T.astype(BF)
        for which, (src, dst) in enumerate(((out_ref, out_hbm), (dq_ref, dq_hbm))):
            copy = pltpu.make_async_copy(
                src.at[i], dst.at[:, pl.ds(h * part, part)], sems.at[which, i]
            )
            copy.start()
            copies.append(copy)
        dkv_ref[0, :, cols(i)] = dot(score_grad[:n], q_rows, 1, 0) * SCALE
        dkv_ref[1, :, cols(i)] = dot(weights_bf[:n], g_rows, 1, 0)
    for copy in copies:
        copy.wait()


def owner_of(ref):
    owners = ref[...]
    lane = lax.broadcasted_iota(jnp.int32, owners.shape, 1)
    mine = jnp.where(lane == lax.axis_index("trunk"), owners, 0)
    return jnp.sum(mine.astype(F32), axis=1, keepdims=True)


def pick_kernel(near_ref, far_ref, *refs, offsets):
    count = len(refs) // 2
    me = lax.axis_index("branch")
    half = near_ref.shape[0]
    for owner_ref, out_ref in zip(refs[:count], refs[count:]):
        owner = owner_of(owner_ref)
        for which in range(out_ref.shape[0]):
            total = jnp.zeros(out_ref.shape[1:], F32)
            for p, offset in enumerate(offsets):
                ref = near_ref if p < half else far_ref
                hit = owner == (me ^ offset).astype(F32)
                total = jnp.where(hit, ref[p % half, which].astype(F32), total)
            out_ref[which] = total.astype(BF)


def split_kernel(*refs, keeps, sends):
    send_ref, keep_ref = refs[-2:]
    count = (len(refs) - 2) // 2
    me = lax.axis_index("branch")
    owners = [owner_of(ref) for ref in refs[:count]]
    for which in range(keep_ref.shape[1]):
        parts = [ref[which].astype(F32) for ref in refs[count:-2]]
        for out_ref, offsets in ((keep_ref, keeps), (send_ref, sends)):
            for i, offset in enumerate(offsets):
                total = jnp.zeros(parts[0].shape, F32)
                for owner, part in zip(owners, parts):
                    hit = owner == (me ^ offset).astype(F32)
                    total = total + jnp.where(hit, part, 0.0)
                out_ref[i, which] = total.astype(out_ref.dtype)


def fold_kernel(kept_ref, got_ref, *out_refs, places):
    for out_ref, where in zip(out_refs, places):
        for i, p in enumerate(where):
            out_ref[i] = (kept_ref[p] + got_ref[p].astype(F32)).astype(out_ref.dtype)


def combine_kernel(next_ref, *refs):
    out_ref = refs[-1]
    first = 0
    for ref in refs[:-1]:
        some = slice(first, first + ref.shape[2])
        for which in range(out_ref.shape[1]):
            out_ref[:, which, some] = ref[which] + next_ref[which, :, some].astype(F32)
        first += ref.shape[2]


def on_device(queries, keys_values, out_grad, trunk_kv, branch_of, branch_reach, ancestors):
    depths = lax.axis_size("trunk")
    n_branch = lax.axis_size("branch")
    n, width = queries.shape[1:]
    seg_len, kv_width = trunk_kv.shape[3:]
    heads = kv_width // DH
    seg_shape = trunk_kv.shape[2:]
    stats_shape = ((heads, 8, n * GROUP), F32)
    bias_shape = ((n, n), F32)
    tbias_shape = ((depths * seg_len, n), F32)
    assert branch_reach.shape[1] < 256 and n_branch & (n_branch - 1) == 0

    bits = [1 << i for i in range(n_branch.bit_length() - 1)][::-1]
    bits = GATHER_FIRST + [x for x in bits if x not in GATHER_FIRST]
    offsets, bit = [0], bits[0]
    far = swap(trunk_kv[0], "branch", bit)
    offsets = offsets + [bit ^ o for o in offsets]
    own_kv = keys_values[0].reshape(n, 2 * kv_width)
    ids, own_owners, q, g, near, payload, tbias = call(
        prepare_kernel,
        [
            ((1, n), jnp.int32), ((1, depths), jnp.int32), ((n, width), BF), ((n, width), BF),
            ((1,) + seg_shape, BF), ((n + PACK, 2 * kv_width), BF), tbias_shape,
        ],
        branch_of, branch_reach, ancestors[0], queries[0], out_grad[0], trunk_kv[0], own_kv,
        hbm=6,
        scratch=[pltpu.VMEM(branch_reach.shape, jnp.int32), pltpu.SemaphoreType.DMA((6,))],
    )
    earlier = ring(payload, "branch", 1)
    owners = [own_owners]
    for k in range(1, depths):
        owners.append(swap(own_owners, "trunk", k))
    for step, bit in enumerate(bits[1:], 1):
        (near,) = call(join_kernel, [((2 * near.shape[0],) + seg_shape, BF)], near, far)
        far = swap(near, "branch", bit)
        offsets = offsets + [bit ^ o for o in offsets]
    stats0, obias = call(own_kernel, [stats_shape, bias_shape], ids, q, g, payload)
    stats1, ebias = call(earlier_kernel, [stats_shape, bias_shape], ids, q, g, earlier, stats0)
    picked = call(
        functools.partial(pick_kernel, offsets=offsets), [(seg_shape, BF)] * depths,
        near, far, *owners,
    )
    segs = [picked[0]]
    for k in range(1, depths):
        segs.append(swap(picked[k], "trunk", k))
    final, *dsegs = call(
        trunk_kernel, [stats_shape] + [(seg_shape, BF)] * depths,
        q, g, stats1, tbias, *segs,
    )
    returned = [dsegs[0]]
    for k in range(1, depths):
        returned.append(swap(dsegs[k], "trunk", k))
    (earlier_part,) = call(
        earlier_grad_kernel, [((2, n, kv_width), BF)],
        q, g, final, earlier, ebias,
    )
    from_next = ring(earlier_part, "branch", -1)
    keeps = list(range(n_branch))
    order = [1 << i for i in range(n_branch.bit_length() - 1)]
    order = SCATTER_FIRST + [x for x in order if x not in SCATTER_FIRST]
    order = [x for x in order if x < n_branch]
    for step, bit in enumerate(order):
        places = [[i for i, o in enumerate(keeps) if not o & bit]]
        places += [[i for i, o in enumerate(keeps) if o & bit]]
        sends = [keeps[i] for i in places[1]]
        keeps = [keeps[i] for i in places[0]]
        sends = [o ^ bit for o in sends]
        assert sends == keeps
        half = (len(keeps),) + seg_shape
        outs = [(half, BF), (half, F32)]
        if step == 0:
            send, kept = call(
                functools.partial(split_kernel, keeps=keeps, sends=[o ^ bit for o in keeps]),
                outs, *owners, *returned,
            )
        else:
            send, kept = call(functools.partial(fold_kernel, places=places[::-1]), outs, kept, got)
        got = swap(send, "branch", bit)
    (trunk_grad,) = call(
        functools.partial(fold_kernel, places=[[0]]),
        [((1,) + seg_shape, F32)], kept, got,
    )
    own_parts, outputs = [], []
    halves = 2
    for part in range(halves):
        some = list(range(heads))[part * heads // halves : (part + 1) * heads // halves]
        *outputs, own_part = call(
            functools.partial(rest_kernel, some=some, aliased=part > 0),
            [((n, width), BF), ((n, width), BF), ((2, n, len(some) * DH), F32)],
            *outputs, q, g, final, earlier, payload, obias, ebias, tbias, *segs,
            hbm=len(outputs), hbm_outs=2, aliases={i: i for i in range(len(outputs))},
            scratch=[
                pltpu.VMEM((len(some), n, width // heads), BF),
                pltpu.VMEM((len(some), n, width // heads), BF),
                pltpu.SemaphoreType.DMA((2, len(some))),
            ],
        )
        own_parts.append(own_part)
    attended, query_grad = outputs
    (kv_grad,) = call(combine_kernel, [((n, 2, kv_width), F32)], from_next, *own_parts)
    kv_grad = kv_grad[None]
    trunk_grad = trunk_grad[None]
    return (attended[None], query_grad[None], kv_grad, trunk_grad)


def solution(mesh):
    return jax.shard_map(
        on_device,
        mesh=mesh,
        in_specs=(
            P("trunk", "branch", None),
            P("trunk", "branch", None, None),
            P("trunk", "branch", None),
            P("trunk", "branch", None, None, None),
            P("trunk", "branch"),
            P("trunk", None),
            P("trunk", "branch", None),
        ),
        out_specs=(
            P("trunk", "branch", None),
            P("trunk", "branch", None),
            P("trunk", "branch", None, None),
            P("trunk", "branch", None, None, None),
        ),
        check_vma=False,
    )
```

```python
import functools
import math

import jax
import jax.numpy as jnp
from jax import lax
from jax.experimental import pallas as pl
from jax.experimental.pallas import tpu as pltpu
from jax.sharding import PartitionSpec as P


HQ = 32
KVH = 4
DH = 128
GROUP = HQ // KVH
SCALE = 1.0 / math.sqrt(DH)
LOG2E = 1.0 / math.log(2.0)
BF = jnp.bfloat16
F32 = jnp.float32
PACK = 16
CHAIN_F = True
CHAIN_R = True
REST_BOUNDS = [2]
VMEM_LIMIT = 24 * 1024 * 1024


def ring(block, axis, distance, chain):
    size = lax.axis_size(axis)
    route = [(i, (i + distance) % size) for i in range(size)]
    if chain:
        route = [(i, j) for i, j in route if j == i + distance]
    return lax.ppermute(block, axis, route)


def swap(block, axis, k):
    if k == 0:
        return block
    return lax.ppermute(block, axis, [(i, i ^ k) for i in range(lax.axis_size(axis))])


def dot(a, b, ca, cb):
    return lax.dot_general(a, b, (((ca,), (cb,)), ((), ())), preferred_element_type=F32)


def head_rows(ref, h):
    first = h * GROUP
    return jnp.concatenate(
        [ref[:, (first + r) * DH : (first + r + 1) * DH] for r in range(GROUP)], axis=0
    )


def tile_heads(x):
    return jnp.concatenate([x] * GROUP, axis=1)


def as_bias(ok):
    return jnp.where(ok, 0.0, -1e30).astype(F32)


def cols(h):
    return slice(h * DH, (h + 1) * DH)


def call(kernel, outs, *args, hbm=0, hbm_outs=0, scratch=(), aliases={}):
    vspec = pl.BlockSpec(memory_space=pltpu.VMEM)
    hspec = pl.BlockSpec(memory_space=pltpu.HBM)
    places = [pltpu.HBM] * hbm + [pltpu.VMEM] * (len(args) - hbm)
    args = [pltpu.with_memory_space_constraint(a, p) for a, p in zip(args, places)]
    shapes = [jax.ShapeDtypeStruct(shape, dtype) for shape, dtype in outs[:hbm_outs]]
    shapes += [pltpu.VMEM(shape, dtype) for shape, dtype in outs[hbm_outs:]]
    return pl.pallas_call(
        kernel,
        in_specs=[hspec] * hbm + [vspec] * (len(args) - hbm),
        out_specs=[hspec] * hbm_outs + [vspec] * (len(outs) - hbm_outs),
        out_shape=shapes,
        scratch_shapes=scratch,
        input_output_aliases=aliases,
        compiler_params=pltpu.CompilerParams(vmem_limit_bytes=VMEM_LIMIT),
        cost_estimate=pl.CostEstimate(flops=10**8, transcendentals=0, bytes_accessed=10**5),
    )(*args)


def join_kernel(*refs):
    for i, ref in enumerate(refs[:-1]):
        refs[-1][i] = ref[0]


def pack_kernel(
    ids_hbm, owners_hbm, seg_hbm, kv_ref, ids_ref, owners_ref, seg_ref, payload_ref, sems
):
    pairs = ((ids_hbm, ids_ref), (owners_hbm, owners_ref), (seg_hbm, seg_ref))
    copies = [pltpu.make_async_copy(src, dst, sems.at[i]) for i, (src, dst) in enumerate(pairs)]
    for copy in copies:
        copy.start()
    n = kv_ref.shape[0]
    payload_ref[:n] = kv_ref[...]
    payload_ref[n:] = jnp.zeros((PACK, kv_ref.shape[1]), BF)
    for copy in copies:
        copy.wait()
    tags = jnp.broadcast_to((ids_ref[...] + 1).astype(F32), (PACK, n))
    payload_ref[n:, 0:n] = tags.astype(BF)


def scored(keys, values, q_rows, g_rows, bias):
    return dot(keys, q_rows, 1, 1) * (SCALE * LOG2E) + bias, dot(values, g_rows, 1, 1)


def own_kernel(
    reach_hbm, q_hbm, g_hbm, ids_ref, kv_ref,
    q_ref, g_ref, stats_ref, bias_ref, tbias_ref, reach_ref, sems,
):
    n = q_ref.shape[0]
    heads = stats_ref.shape[0]
    part = GROUP * DH
    first = pltpu.make_async_copy(reach_hbm, reach_ref, sems.at[2, 0])
    first.start()
    copies = []
    for h in range(heads):
        some = pl.ds(h * part, part)
        for i, (src, dst) in enumerate(((q_hbm, q_ref), (g_hbm, g_ref))):
            copy = pltpu.make_async_copy(src.at[:, some], dst.at[:, some], sems.at[i, h])
            copy.start()
            copies.append(copy)
    ids = ids_ref[...]
    id_cols = jnp.broadcast_to(ids.astype(F32), (n, n))
    k_idx = lax.broadcasted_iota(jnp.int32, (n, n), 0)
    q_idx = lax.broadcasted_iota(jnp.int32, (n, n), 1)
    bias_ref[...] = as_bias((id_cols.T == id_cols) & (k_idx <= q_idx))
    bias = tile_heads(bias_ref[...])
    first.wait()
    reach_row = jnp.zeros((1, n), jnp.int32)
    for b in range(reach_ref.shape[1]):
        reach_row = jnp.where(ids == b, reach_ref[0:1, b : b + 1], reach_row)
    depths = lax.axis_size("trunk")
    seg_len = tbias_ref.shape[0] // depths
    me = lax.axis_index("trunk")
    for k in range(depths):
        row = as_bias((me ^ k) < reach_row)
        tbias_ref[k * seg_len : (k + 1) * seg_len] = jnp.broadcast_to(row, (seg_len, n))
    for h in range(heads):
        copies[2 * h].wait()
        copies[2 * h + 1].wait()
        scores, grad_w = scored(
            kv_ref[:n, cols(h)], kv_ref[:n, cols(h + heads)],
            head_rows(q_ref, h), head_rows(g_ref, h), bias,
        )
        highest = jnp.max(scores, axis=0, keepdims=True)
        expo = jnp.exp2(scores - highest)
        stats_ref[h, 0:1] = highest
        stats_ref[h, 1:2] = jnp.sum(expo, axis=0, keepdims=True)
        stats_ref[h, 2:3] = jnp.sum(expo * grad_w, axis=0, keepdims=True)


def merge(stats_ref, h, scores, grad_w):
    first = stats_ref[h, 0:1]
    highest = jnp.maximum(jnp.max(scores, axis=0, keepdims=True), first)
    expo = jnp.exp2(scores - highest)
    factor = jnp.exp2(first - highest)
    total = jnp.sum(expo, axis=0, keepdims=True) + stats_ref[h, 1:2] * factor
    weighted = jnp.sum(expo * grad_w, axis=0, keepdims=True) + stats_ref[h, 2:3] * factor
    return highest, expo, total, weighted


def earlier_kernel(ids_ref, q_ref, g_ref, kv_ref, stats_ref, merged_ref, bias_ref):
    n = q_ref.shape[0]
    heads = stats_ref.shape[0]
    tag_cols = jnp.broadcast_to(ids_ref[...].astype(F32) + 1.0, (n, n))
    present = (lax.axis_index("branch") > 0).astype(F32)
    earlier_row = kv_ref[n : n + 1, 0:n].astype(F32) * present
    bias_ref[...] = as_bias(jnp.broadcast_to(earlier_row, (n, n)).T == tag_cols)
    bias = tile_heads(bias_ref[...])
    for h in range(heads):
        scores, grad_w = scored(
            kv_ref[:n, cols(h)], kv_ref[:n, cols(h + heads)],
            head_rows(q_ref, h), head_rows(g_ref, h), bias,
        )
        highest, _, total, weighted = merge(stats_ref, h, scores, grad_w)
        merged_ref[h, 0:1] = highest
        merged_ref[h, 1:2] = total
        merged_ref[h, 2:3] = weighted


def trunk_kernel(q_ref, g_ref, stats_ref, tbias_ref, *refs):
    count = len(refs) // 2
    seg_refs, final_ref, dseg_refs = refs[:count], refs[count], refs[count + 1 :]
    seg_len = seg_refs[0].shape[1]
    bias = tile_heads(tbias_ref[...])
    for h in range(stats_ref.shape[0]):
        keys = jnp.concatenate([s[0, :, cols(h)] for s in seg_refs], axis=0)
        values = jnp.concatenate([s[1, :, cols(h)] for s in seg_refs], axis=0)
        q_rows = head_rows(q_ref, h)
        g_rows = head_rows(g_ref, h)
        scores, grad_w = scored(keys, values, q_rows, g_rows, bias)
        highest, expo, total, weighted = merge(stats_ref, h, scores, grad_w)
        inverse = 1.0 / total
        row_mean = weighted * inverse
        weights = expo * inverse
        score_grad = (weights * (grad_w - row_mean)).astype(BF)
        dkey = (dot(score_grad, q_rows, 1, 0) * SCALE).astype(BF)
        dvalue = dot(weights.astype(BF), g_rows, 1, 0).astype(BF)
        for k, ref in enumerate(dseg_refs):
            ref[0, :, cols(h)] = dkey[k * seg_len : (k + 1) * seg_len]
            ref[1, :, cols(h)] = dvalue[k * seg_len : (k + 1) * seg_len]
        final_ref[h, 0:1] = highest
        final_ref[h, 1:2] = inverse
        final_ref[h, 2:3] = row_mean


def finish(final_ref, h, scores, grad_w):
    weights = jnp.exp2(scores - final_ref[h, 0:1]) * final_ref[h, 1:2]
    return weights.astype(BF), (weights * (grad_w - final_ref[h, 2:3])).astype(BF)


def earlier_grad_kernel(q_ref, g_ref, final_ref, kv_ref, bias_ref, dkv_ref):
    n = q_ref.shape[0]
    heads = final_ref.shape[0]
    bias = tile_heads(bias_ref[...])
    for h in range(heads):
        q_rows = head_rows(q_ref, h)
        g_rows = head_rows(g_ref, h)
        scores, grad_w = scored(
            kv_ref[:n, cols(h)], kv_ref[:n, cols(h + heads)], q_rows, g_rows, bias
        )
        weights_bf, score_grad = finish(final_ref, h, scores, grad_w)
        dkv_ref[0, :, cols(h)] = (dot(score_grad, q_rows, 1, 0) * SCALE).astype(BF)
        dkv_ref[1, :, cols(h)] = dot(weights_bf, g_rows, 1, 0).astype(BF)


def rest_kernel(
    *refs, some, aliased
):
    refs = refs[2:] if aliased else refs
    q_ref, g_ref, final_ref, ekv_ref, kv_ref, obias_ref, ebias_ref, tbias_ref = refs[:8]
    seg_refs = refs[8:-6]
    out_hbm, dq_hbm, dkv_ref, out_ref, dq_ref, sems = refs[-6:]
    n = q_ref.shape[0]
    heads = final_ref.shape[0]
    part = GROUP * DH
    bias = tile_heads(jnp.concatenate([obias_ref[...], ebias_ref[...], tbias_ref[...]], axis=0))
    copies, late = [], []
    for i, h in enumerate(some):
        keys = jnp.concatenate(
            [kv_ref[:n, cols(h)], ekv_ref[:n, cols(h)]] + [s[0, :, cols(h)] for s in seg_refs],
            axis=0,
        )
        values = jnp.concatenate(
            [kv_ref[:n, cols(h + heads)], ekv_ref[:n, cols(h + heads)]]
            + [s[1, :, cols(h)] for s in seg_refs],
            axis=0,
        )
        q_rows = head_rows(q_ref, h)
        g_rows = head_rows(g_ref, h)
        scores, grad_w = scored(keys, values, q_rows, g_rows, bias)
        weights_bf, score_grad = finish(final_ref, h, scores, grad_w)
        out_t = dot(values, weights_bf, 0, 0)
        dq_t = dot(keys, score_grad, 0, 0) * SCALE
        for r in range(GROUP):
            rows = slice(r * n, (r + 1) * n)
            out_ref[i, :, cols(r)] = out_t[:, rows].T.astype(BF)
            dq_ref[i, :, cols(r)] = dq_t[:, rows].T.astype(BF)
        for which, (src, dst) in enumerate(((out_ref, out_hbm), (dq_ref, dq_hbm))):
            copy = pltpu.make_async_copy(
                src.at[i], dst.at[:, pl.ds(h * part, part)], sems.at[which, i]
            )
            copy.start()
            copies.append(copy)
        late.append((i, score_grad[:n], q_rows, weights_bf[:n], g_rows))
    for i, score_grad, q_rows, weights_bf, g_rows in late:
        dkv_ref[0, :, cols(i)] = dot(score_grad, q_rows, 1, 0) * SCALE
        dkv_ref[1, :, cols(i)] = dot(weights_bf, g_rows, 1, 0)
    for copy in copies:
        copy.wait()


def owner_of(ref):
    owners = ref[...]
    lane = lax.broadcasted_iota(jnp.int32, owners.shape, 1)
    mine = jnp.where(lane == lax.axis_index("trunk"), owners, 0)
    return jnp.sum(mine.astype(F32), axis=1, keepdims=True)


def pick_kernel(near_ref, far_ref, *refs, offsets):
    count = len(refs) // 2
    me = lax.axis_index("branch")
    half = near_ref.shape[0]
    for owner_ref, out_ref in zip(refs[:count], refs[count:]):
        owner = owner_of(owner_ref)
        for which in range(out_ref.shape[0]):
            total = jnp.zeros(out_ref.shape[1:], F32)
            for p, offset in enumerate(offsets):
                ref = near_ref if p < half else far_ref
                hit = owner == (me ^ offset).astype(F32)
                total = jnp.where(hit, ref[p % half, which].astype(F32), total)
            out_ref[which] = total.astype(BF)


def split_kernel(*refs, keeps, sends):
    send_ref, keep_ref = refs[-2:]
    count = (len(refs) - 2) // 2
    me = lax.axis_index("branch")
    owners = [owner_of(ref) for ref in refs[:count]]
    for which in range(keep_ref.shape[1]):
        parts = [ref[which].astype(F32) for ref in refs[count:-2]]
        for out_ref, offsets in ((keep_ref, keeps), (send_ref, sends)):
            for i, offset in enumerate(offsets):
                total = jnp.zeros(parts[0].shape, F32)
                for owner, part in zip(owners, parts):
                    hit = owner == (me ^ offset).astype(F32)
                    total = total + jnp.where(hit, part, 0.0)
                out_ref[i, which] = total.astype(out_ref.dtype)


def fold_kernel(kept_ref, got_ref, *out_refs):
    for i, out_ref in enumerate(out_refs):
        out_ref[0] = (kept_ref[i] + got_ref[i].astype(F32)).astype(out_ref.dtype)


def last_kernel(total_ref, *refs):
    total = total_ref[...]
    for ref in refs[:-1]:
        total = total + ref[...].astype(F32)
    refs[-1][...] = total


def combine_kernel(next_ref, *refs):
    out_ref = refs[-1]
    first = 0
    for ref in refs[:-1]:
        some = slice(first, first + ref.shape[2])
        for which in range(out_ref.shape[1]):
            out_ref[:, which, some] = ref[which] + next_ref[which, :, some].astype(F32)
        first += ref.shape[2]


def on_device(queries, keys_values, out_grad, trunk_kv, branch_of, branch_reach, ancestors):
    depths = lax.axis_size("trunk")
    n_branch = lax.axis_size("branch")
    n, width = queries.shape[1:]
    seg_len, kv_width = trunk_kv.shape[3:]
    heads = kv_width // DH
    seg_shape = trunk_kv.shape[2:]
    stats_shape = ((heads, 8, n * GROUP), F32)
    bias_shape = ((n, n), F32)
    tbias_shape = ((depths * seg_len, n), F32)
    assert branch_reach.shape[1] < 256 and n_branch & (n_branch - 1) == 0

    steps = list(range(2, n_branch, 2))
    offsets = [0] + steps
    offsets = offsets + [1 ^ o for o in offsets]
    pieces = []
    for k in steps:
        pieces.append(swap(trunk_kv[0], "branch", k))
    own_kv = keys_values[0].reshape(n, 2 * kv_width)
    ids, own_owners, own_seg, payload = call(
        pack_kernel,
        [
            ((1, n), jnp.int32), ((1, depths), jnp.int32),
            ((1,) + seg_shape, BF), ((n + PACK, 2 * kv_width), BF),
        ],
        branch_of, ancestors[0], trunk_kv[0], own_kv,
        hbm=3,
        scratch=[pltpu.SemaphoreType.DMA((3,))],
    )
    earlier = ring(payload, "branch", 1, CHAIN_F)
    owners = [own_owners]
    for k in range(1, depths):
        owners.append(swap(ancestors[0], "trunk", k))
    (near,) = call(join_kernel, [((n_branch // 2,) + seg_shape, BF)], own_seg, *pieces)
    far = swap(near, "branch", 1)
    q, g, stats0, obias, tbias = call(
        own_kernel,
        [((n, width), BF), ((n, width), BF), stats_shape, bias_shape, tbias_shape],
        branch_reach, queries[0], out_grad[0], ids, payload,
        hbm=3,
        scratch=[
            pltpu.VMEM(branch_reach.shape, jnp.int32), pltpu.SemaphoreType.DMA((3, heads)),
        ],
    )
    stats1, ebias = call(earlier_kernel, [stats_shape, bias_shape], ids, q, g, earlier, stats0)
    picked = call(
        functools.partial(pick_kernel, offsets=offsets), [(seg_shape, BF)] * depths,
        near, far, *owners,
    )
    segs = [picked[0]]
    for k in range(1, depths):
        segs.append(swap(picked[k], "trunk", k))
    final, *dsegs = call(
        trunk_kernel, [stats_shape] + [(seg_shape, BF)] * depths,
        q, g, stats1, tbias, *segs,
    )
    returned = [dsegs[0]]
    for k in range(1, depths):
        returned.append(swap(dsegs[k], "trunk", k))
    (earlier_part,) = call(
        earlier_grad_kernel, [((2, n, kv_width), BF)],
        q, g, final, earlier, ebias,
    )
    from_next = ring(earlier_part, "branch", -1, CHAIN_R)
    half, one = (n_branch // 2,) + seg_shape, (1,) + seg_shape
    keeps = [0] + steps
    send, kept = call(
        functools.partial(split_kernel, keeps=keeps, sends=[o ^ 1 for o in keeps]),
        [(half, BF), (half, F32)], *owners, *returned,
    )
    got = swap(send, "branch", 1)
    total, *sends = call(fold_kernel, [(one, F32)] + [(one, BF)] * len(steps), kept, got)
    pieces = []
    for k, send in zip(steps, sends):
        pieces.append(swap(send, "branch", k))
    (trunk_grad,) = call(last_kernel, [(one, F32)], total, *pieces)
    own_parts, outputs = [], []
    bounds = [0] + [min(x, heads) for x in REST_BOUNDS] + [heads]
    for part, (first, end) in enumerate(zip(bounds[:-1], bounds[1:])):
        some = list(range(first, end))
        *outputs, own_part = call(
            functools.partial(rest_kernel, some=some, aliased=part > 0),
            [((n, width), BF), ((n, width), BF), ((2, n, len(some) * DH), F32)],
            *outputs, q, g, final, earlier, payload, obias, ebias, tbias, *segs,
            hbm=len(outputs), hbm_outs=2, aliases={i: i for i in range(len(outputs))},
            scratch=[
                pltpu.VMEM((len(some), n, width // heads), BF),
                pltpu.VMEM((len(some), n, width // heads), BF),
                pltpu.SemaphoreType.DMA((2, len(some))),
            ],
        )
        own_parts.append(own_part)
    attended, query_grad = outputs
    (kv_grad,) = call(combine_kernel, [((n, 2, kv_width), F32)], from_next, *own_parts)
    kv_grad = kv_grad[None]
    trunk_grad = trunk_grad[None]
    return (attended[None], query_grad[None], kv_grad, trunk_grad)


def solution(mesh):
    return jax.shard_map(
        on_device,
        mesh=mesh,
        in_specs=(
            P("trunk", "branch", None),
            P("trunk", "branch", None, None),
            P("trunk", "branch", None),
            P("trunk", "branch", None, None, None),
            P("trunk", "branch"),
            P("trunk", None),
            P("trunk", "branch", None),
        ),
        out_specs=(
            P("trunk", "branch", None),
            P("trunk", "branch", None),
            P("trunk", "branch", None, None),
            P("trunk", "branch", None, None, None),
        ),
        check_vma=False,
    )
```

```python
import functools
import math

import jax
import jax.numpy as jnp
from jax import lax
from jax.experimental import pallas as pl
from jax.experimental.pallas import tpu as pltpu
from jax.sharding import PartitionSpec as P


HQ = 32
KVH = 4
DH = 128
GROUP = HQ // KVH
SCALE = 1.0 / math.sqrt(DH)
LOG2E = 1.0 / math.log(2.0)
BF = jnp.bfloat16
F32 = jnp.float32
PACK = 16
CHAIN_F = True
CHAIN_R = True
REST_BOUNDS = [2]
VMEM_LIMIT = 24 * 1024 * 1024


def ring(block, axis, distance, chain):
    size = lax.axis_size(axis)
    route = [(i, (i + distance) % size) for i in range(size)]
    if chain:
        route = [(i, j) for i, j in route if j == i + distance]
    return lax.ppermute(block, axis, route)


def swap(block, axis, k):
    if k == 0:
        return block
    return lax.ppermute(block, axis, [(i, i ^ k) for i in range(lax.axis_size(axis))])


def dot(a, b, ca, cb):
    return lax.dot_general(a, b, (((ca,), (cb,)), ((), ())), preferred_element_type=F32)


def head_rows(ref, h):
    first = h * GROUP
    return jnp.concatenate(
        [ref[:, (first + r) * DH : (first + r + 1) * DH] for r in range(GROUP)], axis=0
    )


def tile_heads(x):
    return jnp.concatenate([x] * GROUP, axis=1)


def as_bias(ok):
    return jnp.where(ok, 0.0, -1e30).astype(F32)


def cols(h):
    return slice(h * DH, (h + 1) * DH)


def call(kernel, outs, *args, hbm=0, hbm_outs=0, scratch=(), aliases={}):
    vspec = pl.BlockSpec(memory_space=pltpu.VMEM)
    hspec = pl.BlockSpec(memory_space=pltpu.HBM)
    places = [pltpu.HBM] * hbm + [pltpu.VMEM] * (len(args) - hbm)
    args = [pltpu.with_memory_space_constraint(a, p) for a, p in zip(args, places)]
    shapes = [jax.ShapeDtypeStruct(shape, dtype) for shape, dtype in outs[:hbm_outs]]
    shapes += [pltpu.VMEM(shape, dtype) for shape, dtype in outs[hbm_outs:]]
    return pl.pallas_call(
        kernel,
        in_specs=[hspec] * hbm + [vspec] * (len(args) - hbm),
        out_specs=[hspec] * hbm_outs + [vspec] * (len(outs) - hbm_outs),
        out_shape=shapes,
        scratch_shapes=scratch,
        input_output_aliases=aliases,
        compiler_params=pltpu.CompilerParams(vmem_limit_bytes=VMEM_LIMIT),
        cost_estimate=pl.CostEstimate(flops=10**8, transcendentals=0, bytes_accessed=10**5),
    )(*args)


def join_kernel(*refs):
    for i, ref in enumerate(refs[:-1]):
        refs[-1][i] = ref[0]


def pack_kernel(
    ids_hbm, owners_hbm, seg_hbm, reach_hbm, q_hbm, g_hbm, kv_ref,
    ids_ref, owners_ref, seg_ref, reach_ref, q_ref, g_ref, payload_ref, sems,
):
    pairs = (
        (ids_hbm, ids_ref), (owners_hbm, owners_ref), (seg_hbm, seg_ref),
        (reach_hbm, reach_ref), (q_hbm, q_ref), (g_hbm, g_ref),
    )
    copies = [pltpu.make_async_copy(src, dst, sems.at[i]) for i, (src, dst) in enumerate(pairs)]
    for copy in copies:
        copy.start()
    n = kv_ref.shape[0]
    payload_ref[:n] = kv_ref[...]
    payload_ref[n:] = jnp.zeros((PACK, kv_ref.shape[1]), BF)
    for copy in copies:
        copy.wait()
    tags = jnp.broadcast_to((ids_ref[...] + 1).astype(F32), (PACK, n))
    payload_ref[n:, 0:n] = tags.astype(BF)


def scored(keys, values, q_rows, g_rows, bias):
    return dot(keys, q_rows, 1, 1) * (SCALE * LOG2E) + bias, dot(values, g_rows, 1, 1)


def own_kernel(
    reach_ref, ids_ref, kv_ref, q_ref, g_ref, stats_ref, bias_ref, tbias_ref
):
    n = q_ref.shape[0]
    heads = stats_ref.shape[0]
    ids = ids_ref[...]
    id_cols = jnp.broadcast_to(ids.astype(F32), (n, n))
    k_idx = lax.broadcasted_iota(jnp.int32, (n, n), 0)
    q_idx = lax.broadcasted_iota(jnp.int32, (n, n), 1)
    bias_ref[...] = as_bias((id_cols.T == id_cols) & (k_idx <= q_idx))
    bias = tile_heads(bias_ref[...])
    reach_row = jnp.zeros((1, n), jnp.int32)
    for b in range(reach_ref.shape[1]):
        reach_row = jnp.where(ids == b, reach_ref[0:1, b : b + 1], reach_row)
    depths = lax.axis_size("trunk")
    seg_len = tbias_ref.shape[0] // depths
    me = lax.axis_index("trunk")
    for k in range(depths):
        row = as_bias((me ^ k) < reach_row)
        tbias_ref[k * seg_len : (k + 1) * seg_len] = jnp.broadcast_to(row, (seg_len, n))
    for h in range(heads):
        scores, grad_w = scored(
            kv_ref[:n, cols(h)], kv_ref[:n, cols(h + heads)],
            head_rows(q_ref, h), head_rows(g_ref, h), bias,
        )
        highest = jnp.max(scores, axis=0, keepdims=True)
        expo = jnp.exp2(scores - highest)
        stats_ref[h, 0:1] = highest
        stats_ref[h, 1:2] = jnp.sum(expo, axis=0, keepdims=True)
        stats_ref[h, 2:3] = jnp.sum(expo * grad_w, axis=0, keepdims=True)


def merge(stats_ref, h, scores, grad_w):
    first = stats_ref[h, 0:1]
    highest = jnp.maximum(jnp.max(scores, axis=0, keepdims=True), first)
    expo = jnp.exp2(scores - highest)
    factor = jnp.exp2(first - highest)
    total = jnp.sum(expo, axis=0, keepdims=True) + stats_ref[h, 1:2] * factor
    weighted = jnp.sum(expo * grad_w, axis=0, keepdims=True) + stats_ref[h, 2:3] * factor
    return highest, expo, total, weighted


def earlier_kernel(ids_ref, q_ref, g_ref, kv_ref, stats_ref, merged_ref, bias_ref):
    n = q_ref.shape[0]
    heads = stats_ref.shape[0]
    tag_cols = jnp.broadcast_to(ids_ref[...].astype(F32) + 1.0, (n, n))
    present = (lax.axis_index("branch") > 0).astype(F32)
    earlier_row = kv_ref[n : n + 1, 0:n].astype(F32) * present
    bias_ref[...] = as_bias(jnp.broadcast_to(earlier_row, (n, n)).T == tag_cols)
    bias = tile_heads(bias_ref[...])
    for h in range(heads):
        scores, grad_w = scored(
            kv_ref[:n, cols(h)], kv_ref[:n, cols(h + heads)],
            head_rows(q_ref, h), head_rows(g_ref, h), bias,
        )
        highest, _, total, weighted = merge(stats_ref, h, scores, grad_w)
        merged_ref[h, 0:1] = highest
        merged_ref[h, 1:2] = total
        merged_ref[h, 2:3] = weighted


def trunk_kernel(q_ref, g_ref, stats_ref, tbias_ref, *refs):
    count = len(refs) // 2
    seg_refs, final_ref, dseg_refs = refs[:count], refs[count], refs[count + 1 :]
    seg_len = seg_refs[0].shape[1]
    bias = tile_heads(tbias_ref[...])
    for h in range(stats_ref.shape[0]):
        keys = jnp.concatenate([s[0, :, cols(h)] for s in seg_refs], axis=0)
        values = jnp.concatenate([s[1, :, cols(h)] for s in seg_refs], axis=0)
        q_rows = head_rows(q_ref, h)
        g_rows = head_rows(g_ref, h)
        scores, grad_w = scored(keys, values, q_rows, g_rows, bias)
        highest, expo, total, weighted = merge(stats_ref, h, scores, grad_w)
        inverse = 1.0 / total
        row_mean = weighted * inverse
        weights = expo * inverse
        score_grad = (weights * (grad_w - row_mean)).astype(BF)
        dkey = (dot(score_grad, q_rows, 1, 0) * SCALE).astype(BF)
        dvalue = dot(weights.astype(BF), g_rows, 1, 0).astype(BF)
        for k, ref in enumerate(dseg_refs):
            ref[0, :, cols(h)] = dkey[k * seg_len : (k + 1) * seg_len]
            ref[1, :, cols(h)] = dvalue[k * seg_len : (k + 1) * seg_len]
        final_ref[h, 0:1] = highest
        final_ref[h, 1:2] = inverse
        final_ref[h, 2:3] = row_mean


def finish(final_ref, h, scores, grad_w):
    weights = jnp.exp2(scores - final_ref[h, 0:1]) * final_ref[h, 1:2]
    return weights.astype(BF), (weights * (grad_w - final_ref[h, 2:3])).astype(BF)


def earlier_grad_kernel(q_ref, g_ref, final_ref, kv_ref, bias_ref, dkv_ref):
    n = q_ref.shape[0]
    heads = final_ref.shape[0]
    bias = tile_heads(bias_ref[...])
    for h in range(heads):
        q_rows = head_rows(q_ref, h)
        g_rows = head_rows(g_ref, h)
        scores, grad_w = scored(
            kv_ref[:n, cols(h)], kv_ref[:n, cols(h + heads)], q_rows, g_rows, bias
        )
        weights_bf, score_grad = finish(final_ref, h, scores, grad_w)
        dkv_ref[0, :, cols(h)] = (dot(score_grad, q_rows, 1, 0) * SCALE).astype(BF)
        dkv_ref[1, :, cols(h)] = dot(weights_bf, g_rows, 1, 0).astype(BF)


def rest_kernel(
    *refs, some, aliased
):
    refs = refs[2:] if aliased else refs
    q_ref, g_ref, final_ref, ekv_ref, kv_ref, obias_ref, ebias_ref, tbias_ref = refs[:8]
    seg_refs = refs[8:-6]
    out_hbm, dq_hbm, dkv_ref, out_ref, dq_ref, sems = refs[-6:]
    n = q_ref.shape[0]
    heads = final_ref.shape[0]
    part = GROUP * DH
    bias = tile_heads(jnp.concatenate([obias_ref[...], ebias_ref[...], tbias_ref[...]], axis=0))
    copies, late = [], []
    for i, h in enumerate(some):
        keys = jnp.concatenate(
            [kv_ref[:n, cols(h)], ekv_ref[:n, cols(h)]] + [s[0, :, cols(h)] for s in seg_refs],
            axis=0,
        )
        values = jnp.concatenate(
            [kv_ref[:n, cols(h + heads)], ekv_ref[:n, cols(h + heads)]]
            + [s[1, :, cols(h)] for s in seg_refs],
            axis=0,
        )
        q_rows = head_rows(q_ref, h)
        g_rows = head_rows(g_ref, h)
        scores, grad_w = scored(keys, values, q_rows, g_rows, bias)
        weights_bf, score_grad = finish(final_ref, h, scores, grad_w)
        out_t = dot(values, weights_bf, 0, 0)
        dq_t = dot(keys, score_grad, 0, 0) * SCALE
        for r in range(GROUP):
            rows = slice(r * n, (r + 1) * n)
            out_ref[i, :, cols(r)] = out_t[:, rows].T.astype(BF)
            dq_ref[i, :, cols(r)] = dq_t[:, rows].T.astype(BF)
        for which, (src, dst) in enumerate(((out_ref, out_hbm), (dq_ref, dq_hbm))):
            copy = pltpu.make_async_copy(
                src.at[i], dst.at[:, pl.ds(h * part, part)], sems.at[which, i]
            )
            copy.start()
            copies.append(copy)
        late.append((i, score_grad[:n], q_rows, weights_bf[:n], g_rows))
    for i, score_grad, q_rows, weights_bf, g_rows in late:
        dkv_ref[0, :, cols(i)] = dot(score_grad, q_rows, 1, 0) * SCALE
        dkv_ref[1, :, cols(i)] = dot(weights_bf, g_rows, 1, 0)
    for copy in copies:
        copy.wait()


def owner_of(ref):
    owners = ref[...]
    lane = lax.broadcasted_iota(jnp.int32, owners.shape, 1)
    mine = jnp.where(lane == lax.axis_index("trunk"), owners, 0)
    return jnp.sum(mine.astype(F32), axis=1, keepdims=True)


def pick_kernel(near_ref, far_ref, *refs, offsets):
    count = len(refs) // 2
    me = lax.axis_index("branch")
    half = near_ref.shape[0]
    for owner_ref, out_ref in zip(refs[:count], refs[count:]):
        owner = owner_of(owner_ref)
        for which in range(out_ref.shape[0]):
            total = jnp.zeros(out_ref.shape[1:], F32)
            for p, offset in enumerate(offsets):
                ref = near_ref if p < half else far_ref
                hit = owner == (me ^ offset).astype(F32)
                total = jnp.where(hit, ref[p % half, which].astype(F32), total)
            out_ref[which] = total.astype(BF)


def split_kernel(*refs, keeps, sends):
    send_ref, keep_ref = refs[-2:]
    count = (len(refs) - 2) // 2
    me = lax.axis_index("branch")
    owners = [owner_of(ref) for ref in refs[:count]]
    for which in range(keep_ref.shape[1]):
        parts = [ref[which].astype(F32) for ref in refs[count:-2]]
        for out_ref, offsets in ((keep_ref, keeps), (send_ref, sends)):
            for i, offset in enumerate(offsets):
                total = jnp.zeros(parts[0].shape, F32)
                for owner, part in zip(owners, parts):
                    hit = owner == (me ^ offset).astype(F32)
                    total = total + jnp.where(hit, part, 0.0)
                out_ref[i, which] = total.astype(out_ref.dtype)


def fold_kernel(kept_ref, got_ref, *out_refs):
    for i, out_ref in enumerate(out_refs):
        out_ref[0] = (kept_ref[i] + got_ref[i].astype(F32)).astype(out_ref.dtype)


def last_kernel(total_ref, *refs):
    total = total_ref[...]
    for ref in refs[:-1]:
        total = total + ref[...].astype(F32)
    refs[-1][...] = total


def combine_kernel(next_ref, *refs):
    out_ref = refs[-1]
    first = 0
    for ref in refs[:-1]:
        some = slice(first, first + ref.shape[2])
        for which in range(out_ref.shape[1]):
            out_ref[:, which, some] = ref[which] + next_ref[which, :, some].astype(F32)
        first += ref.shape[2]


def on_device(queries, keys_values, out_grad, trunk_kv, branch_of, branch_reach, ancestors):
    depths = lax.axis_size("trunk")
    n_branch = lax.axis_size("branch")
    n, width = queries.shape[1:]
    seg_len, kv_width = trunk_kv.shape[3:]
    heads = kv_width // DH
    seg_shape = trunk_kv.shape[2:]
    stats_shape = ((heads, 8, n * GROUP), F32)
    bias_shape = ((n, n), F32)
    tbias_shape = ((depths * seg_len, n), F32)
    assert branch_reach.shape[1] < 256 and n_branch & (n_branch - 1) == 0

    steps = list(range(2, n_branch, 2))
    offsets = [0] + steps
    offsets = offsets + [1 ^ o for o in offsets]
    pieces = []
    for k in steps:
        pieces.append(swap(trunk_kv[0], "branch", k))
    own_kv = keys_values[0].reshape(n, 2 * kv_width)
    ids, own_owners, own_seg, reach, q, g, payload = call(
        pack_kernel,
        [
            ((1, n), jnp.int32), ((1, depths), jnp.int32), ((1,) + seg_shape, BF),
            (branch_reach.shape, jnp.int32), ((n, width), BF), ((n, width), BF),
            ((n + PACK, 2 * kv_width), BF),
        ],
        branch_of, ancestors[0], trunk_kv[0], branch_reach, queries[0], out_grad[0], own_kv,
        hbm=6,
        scratch=[pltpu.SemaphoreType.DMA((6,))],
    )
    earlier = ring(payload, "branch", 1, CHAIN_F)
    owners = [own_owners]
    for k in range(1, depths):
        owners.append(swap(ancestors[0], "trunk", k))
    (near,) = call(join_kernel, [((n_branch // 2,) + seg_shape, BF)], own_seg, *pieces)
    far = swap(near, "branch", 1)
    stats0, obias, tbias = call(
        own_kernel, [stats_shape, bias_shape, tbias_shape], reach, ids, payload, q, g
    )
    stats1, ebias = call(earlier_kernel, [stats_shape, bias_shape], ids, q, g, earlier, stats0)
    picked = call(
        functools.partial(pick_kernel, offsets=offsets), [(seg_shape, BF)] * depths,
        near, far, *owners,
    )
    segs = [picked[0]]
    for k in range(1, depths):
        segs.append(swap(picked[k], "trunk", k))
    final, *dsegs = call(
        trunk_kernel, [stats_shape] + [(seg_shape, BF)] * depths,
        q, g, stats1, tbias, *segs,
    )
    returned = [dsegs[0]]
    for k in range(1, depths):
        returned.append(swap(dsegs[k], "trunk", k))
    (earlier_part,) = call(
        earlier_grad_kernel, [((2, n, kv_width), BF)],
        q, g, final, earlier, ebias,
    )
    from_next = ring(earlier_part, "branch", -1, CHAIN_R)
    half, one = (n_branch // 2,) + seg_shape, (1,) + seg_shape
    keeps = [0] + steps
    send, kept = call(
        functools.partial(split_kernel, keeps=keeps, sends=[o ^ 1 for o in keeps]),
        [(half, BF), (half, F32)], *owners, *returned,
    )
    got = swap(send, "branch", 1)
    total, *sends = call(fold_kernel, [(one, F32)] + [(one, BF)] * len(steps), kept, got)
    pieces = []
    for k, send in zip(steps, sends):
        pieces.append(swap(send, "branch", k))
    (trunk_grad,) = call(last_kernel, [(one, F32)], total, *pieces)
    own_parts, outputs = [], []
    bounds = [0] + [min(x, heads) for x in REST_BOUNDS] + [heads]
    for part, (first, end) in enumerate(zip(bounds[:-1], bounds[1:])):
        some = list(range(first, end))
        *outputs, own_part = call(
            functools.partial(rest_kernel, some=some, aliased=part > 0),
            [((n, width), BF), ((n, width), BF), ((2, n, len(some) * DH), F32)],
            *outputs, q, g, final, earlier, payload, obias, ebias, tbias, *segs,
            hbm=len(outputs), hbm_outs=2, aliases={i: i for i in range(len(outputs))},
            scratch=[
                pltpu.VMEM((len(some), n, width // heads), BF),
                pltpu.VMEM((len(some), n, width // heads), BF),
                pltpu.SemaphoreType.DMA((2, len(some))),
            ],
        )
        own_parts.append(own_part)
    attended, query_grad = outputs
    (kv_grad,) = call(combine_kernel, [((n, 2, kv_width), F32)], from_next, *own_parts)
    kv_grad = kv_grad[None]
    trunk_grad = trunk_grad[None]
    return (attended[None], query_grad[None], kv_grad, trunk_grad)


def solution(mesh):
    return jax.shard_map(
        on_device,
        mesh=mesh,
        in_specs=(
            P("trunk", "branch", None),
            P("trunk", "branch", None, None),
            P("trunk", "branch", None),
            P("trunk", "branch", None, None, None),
            P("trunk", "branch"),
            P("trunk", None),
            P("trunk", "branch", None),
        ),
        out_specs=(
            P("trunk", "branch", None),
            P("trunk", "branch", None),
            P("trunk", "branch", None, None),
            P("trunk", "branch", None, None, None),
        ),
        check_vma=False,
    )
```
